32 devices in a mesh: row: 4 (over y, core), col: 8 (over z, x).
Axes of the slice: x: 2, y: 2, z: 4, core: 2. Of those that a mesh axis runs over, the one named last changes fastest.
Arguments:
- matrix: bfloat16 [6144, 6144], P('row', 'col'), as said below
- polar_factor: bfloat16 [6144, 6144], P('row', 'col'), as said below
- start_basis: bfloat16 [6144, 6144], P('row', 'col'), may hold values from -0.078125 to 0.078125
Outputs:
- gram_halves: float32 [3072, 6144], P('row', 'col')
- projected: float32 [3072, 6144], P('row', 'col')
The draws below stay inside these ranges and needn't reach their ends.
Inputs may be any that keep to these rules, and one draw needn't show every extreme that they name: `matrix`: symmetric. `polar_factor`: symmetric.
All inputs are finite; a program needn't handle non-finite values.
Results may differ from the reference program's by a relative error of at most 0.017.
Values may be sent and summed in bfloat16 or wider, within the bound.
A program may use at most 128 MiB of HBM per device.

```python
import jax
import jax.numpy as jnp
from jax import lax

N = 6144
K = 3072
BLOCK_ROWS = 1536
HALF_BLOCK = 384
N_ROW = 4
N_COL = 8


def spectral_parts(key):
    base = jax.random.fold_in(key, 7)
    first, second, third = jax.random.split(base, 3)
    normal_draw = jax.random.normal(first, (N, N), jnp.float32)
    orthogonal, unused = jnp.linalg.qr(normal_draw)
    magnitude = jax.random.uniform(second, (N,), jnp.float32, 0.2, 2.0)
    signs = jnp.where(jnp.arange(N) < K, 1.0, -1.0).astype(jnp.float32)
    errors = jax.random.uniform(third, (N,), jnp.float32, 0.0, 0.3)
    return (orthogonal, signs * magnitude, signs * (1.0 - errors))


def symmetric_from(orthogonal, values):
    built = jnp.dot(orthogonal * values[None, :], orthogonal.T, precision=lax.Precision.HIGHEST)
    return 0.5 * (built + built.T)


def draw_matrix(key, part):
    orthogonal, eigen, polar = spectral_parts(key)
    return symmetric_from(orthogonal, eigen).astype(jnp.bfloat16)


def draw_polar_factor(key, part):
    orthogonal, eigen, polar = spectral_parts(key)
    return symmetric_from(orthogonal, polar).astype(jnp.bfloat16)


def block_scale(own_key, shape, pieces, smallest, top_value):
    gain, own = 1.0, jax.random.fold_in(own_key, 6)
    for dim, blocks in pieces:
        heights = jnp.exp(jax.random.uniform(jax.random.fold_in(own, dim), (blocks,), jnp.float32, smallest / len(pieces), top_value / len(pieces)))
        gain = gain * jnp.repeat(heights, shape[dim] // blocks).reshape([-1 if axis == dim else 1 for axis in range(len(shape))])
    return gain


def noise(stream_key, dims, width, bound, cuts=(), dtype=jnp.bfloat16):
    factor_of = block_scale(stream_key, dims, cuts, -0.22, 0.18) if cuts else 1.0
    array = jax.random.normal(stream_key, dims, jnp.float32) * width * factor_of
    return jnp.minimum(jnp.maximum(array, -bound), bound).astype(dtype)


def setup_inputs(seed: int = 0) -> dict:
    splits = jax.random.split(jax.random.key(seed), 4)
    matrix = draw_matrix(jax.random.fold_in(splits[3], 71), 0)
    polar_factor = draw_polar_factor(jax.random.fold_in(splits[3], 71), 0)
    start_basis = noise(splits[2], (N, 2 * K), N ** -0.5, 0.078125, ((0, 4), (1, 8)))
    return dict(matrix=matrix, polar_factor=polar_factor, start_basis=start_basis)


def add_block(running, blocks):
    left, right = blocks
    term = jnp.dot(left.T.astype(jnp.float32), right.astype(jnp.float32), preferred_element_type=jnp.float32).astype(jnp.bfloat16)
    term = lax.optimization_barrier(term)
    return (running + term.astype(jnp.float32), None)

def reference(matrix, polar_factor, start_basis):
    product = jnp.dot(polar_factor.astype(jnp.float32), start_basis.astype(jnp.float32), preferred_element_type=jnp.float32)
    signs = jnp.where(jnp.arange(2 * K) // HALF_BLOCK % 2 == 0, 1.0, -1.0).astype(jnp.float32)
    basis = ((start_basis.astype(jnp.float32) + signs * product) * 0.5).astype(jnp.bfloat16)
    image = jnp.dot(matrix.astype(jnp.float32), basis.astype(jnp.float32), preferred_element_type=jnp.float32).astype(jnp.bfloat16)
    basis_split = basis.reshape(N, N_COL, 2, HALF_BLOCK)
    image_split = image.reshape(N, N_COL, 2, HALF_BLOCK)
    grams = []
    projections = []
    for which in range(2):
        basis_half = basis_split[:, :, which, :].reshape(N, K)
        image_half = image_split[:, :, which, :].reshape(N, K)
        joined = jnp.concatenate([basis_half, image_half], axis=1)
        left_blocks = basis_half.reshape(N_ROW, BLOCK_ROWS, K)
        right_blocks = joined.reshape(N_ROW, BLOCK_ROWS, 2 * K)
        summed, unused = lax.scan(add_block, jnp.zeros((K, 2 * K), jnp.float32), (left_blocks, right_blocks))
        grams.append(summed[:, :K].reshape(K, N_COL, HALF_BLOCK))
        projections.append(summed[:, K:].reshape(K, N_COL, HALF_BLOCK))
    gram_halves = jnp.stack(grams, axis=2).reshape(K, 2 * K)
    projected = jnp.stack(projections, axis=2).reshape(K, 2 * K)
    return (gram_halves, projected)
```

```python
import jax
import jax.numpy as jnp
from jax import lax
from jax.experimental import pallas as pl
from jax.experimental.pallas import tpu as pltpu
from jax.sharding import PartitionSpec as P

MESH = pl.DeviceIdType.MESH


def ring_member(place, count):
    return jnp.where(place < count // 2, 2 * place, 2 * (count - 1 - place) + 1)


def ring_pairs(count):
    order = list(range(0, count, 2)) + list(range(count - 1, 0, -2))
    up = [(order[i], order[(i + 1) % count]) for i in range(count)]
    return up, [(b, a) for a, b in up]


def ring(first, second, count, consume, state, tie_from, hold=None):
    here = lax.axis_index("col")
    place = jnp.where(here % 2 == 0, here // 2, count - 1 - here // 2)
    up, down = ring_pairs(count)
    seen = []
    for step in range(count):
        if hold is not None and step == 2:
            first, second, _ = lax.optimization_barrier((first, second, hold))
        if step < count - 1:
            next_first = lax.ppermute(first, "col", up)
            next_second = lax.ppermute(second, "col", down)
        owner_first = ring_member(lax.rem(place - step + count, count), count)
        owner_second = ring_member(lax.rem(place + step, count), count)
        state = consume(state, first, owner_first, second, owner_second)
        seen.append(first)
        if tie_from <= step < count - 1:
            next_first, next_second, state = lax.optimization_barrier(
                (next_first, next_second, state)
            )
        first, second = next_first, next_second
    return state, seen


def block_row_product(block, columns, count, half_rows, tie_from, hold=None):
    depth = block.shape[1]

    def consume(state, top, owner_top, bottom, owner_bottom):
        pieces = []
        for total, piece, owner in ((state[0], top, owner_top), (state[1], bottom, owner_bottom)):
            rows = lax.dynamic_slice_in_dim(columns, owner * depth, depth, 0)
            term = jnp.dot(piece, rows, preferred_element_type=jnp.float32)
            pieces.append(term if total is None else total + term)
        return tuple(pieces)

    return ring(
        block[:half_rows], block[half_rows:], count, consume, (None, None), tie_from, hold
    )


def transposed_product(left, right):
    return lax.dot_general(
        left, right, (((0,), (0,)), ((), ())), preferred_element_type=jnp.float32
    )


def ring_plan(matrix, polar_factor, start_basis):
    local_rows, width = start_basis.shape
    count = lax.axis_size("col")
    half = width // 2
    half_rows = local_rows // 2
    sign = jnp.where(jnp.arange(width) < half, 1.0, -1.0).astype(jnp.float32)

    start_cols = lax.all_gather(start_basis, "row", axis=0, tiled=True)
    (top, bottom), polar_seen = block_row_product(
        polar_factor, start_cols, count, half_rows, count // 2
    )
    product = jnp.concatenate([top, bottom], axis=0)
    basis = ((start_basis.astype(jnp.float32) + sign * product) * 0.5).astype(jnp.bfloat16)
    basis_cols = lax.all_gather(basis, "row", axis=0, tiled=True)

    def keep(state, first, owner_first, second, owner_second):
        return (
            lax.dynamic_update_slice_in_dim(state[0], first, owner_first * half, 1),
            lax.dynamic_update_slice_in_dim(state[1], second, owner_second * half, 1),
        )

    empty = jnp.zeros((local_rows, half * count), jnp.bfloat16)
    lefts, seen = ring(basis[:, :half], basis[:, half:], count, keep, (empty, empty), count)

    matrix, _ = lax.optimization_barrier((matrix, polar_seen[-1]))
    halves, _ = block_row_product(
        matrix, basis_cols, count, half_rows, 2, seen[count // 2]
    )
    image = jnp.concatenate(halves, axis=0).astype(jnp.bfloat16)

    def summed(right):
        terms = [
            transposed_product(lefts[0], right[:, :half]),
            transposed_product(lefts[1], right[:, half:]),
        ]
        return lax.psum_scatter(
            jnp.concatenate(terms, axis=1).astype(jnp.bfloat16),
            "row",
            scatter_dimension=0,
            tiled=True,
        ).astype(jnp.float32)

    return summed(basis), summed(image)


def wait_for(ref, sem):
    pltpu.make_async_copy(ref, ref, sem).wait()


def plane_kernel(
    m_ref, p_ref, s_ref, gram_ref, proj_ref, stage_ref,
    panel, line, cols, acc, give_x, got_x, give_y, got_y, got_far,
    start_send, start_recv, far_send, far_recv, ring_send, ring_recv, core_send, core_recv,
    extra_send, extra_recv, load_sem, y_send, y_recv, x_send, x_recv, half_send, half_recv,
    line_send, line_recv, pair_send, pair_recv, term_send, term_recv, out_send, out_recv,
):
    rows, w = s_ref.shape
    half = w // 2
    row, col = lax.axis_index("row"), lax.axis_index("col")
    layers = line.shape[0] // 2
    y, c, z, x = row // 2, lax.rem(row, 2), col // 2, lax.rem(col, 2)
    q = row
    f32, bf16 = jnp.float32, jnp.bfloat16

    def mod(value, count):
        return lax.rem(value + count, count)

    def place(a, b, d, e):
        return (2 * a + b, 2 * d + e)

    across_x = place(y, c, z, 1 - x)
    across_y = place(1 - y, c, z, x)
    partner = place(y, 1 - c, z, x)
    crossed = place(y, 1 - c, z, 1 - x)
    above = place(y, c, mod(z + 1, layers), x)
    below = place(y, c, mod(z - 1, layers), x)

    def remote(src, dst, send, recv, target):
        return pltpu.make_async_remote_copy(
            src_ref=src, dst_ref=dst, send_sem=send, recv_sem=recv,
            device_id=target, device_id_type=MESH,
        )

    barrier = pltpu.get_barrier_semaphore()
    everyone = (across_x, across_y, partner, crossed, above, below)
    for target in everyone:
        pl.semaphore_signal(barrier, inc=1, device_id=target, device_id_type=MESH)
    pl.semaphore_wait(barrier, len(everyone))

    offset = mod(z - q, layers)
    pick = jnp.where(offset < 2, 0, jnp.where(offset == 2, y, 1))
    chosen = pl.ds(pl.multiple_of(mod(x + pick, 2) * w, w), w)
    unchosen = pl.ds(pl.multiple_of((1 - x) * w, w), w)

    def slot(step, core):
        return mod(z - step - (2 * y + core) + layers, layers)


    def block_home(job):
        return panel if job == 0 else stage_ref

    def block_source(job, step):
        if step == 0:
            return (p_ref if job == 0 else m_ref).at[chosen]
        return block_home(job).at[c, slot(step, c)]

    def ring_copy(job, step):
        return remote(
            block_source(job, step), block_home(job).at[c, slot(step, c)],
            ring_send.at[job, step], ring_recv.at[job, step], above,
        )

    def core_copy(job, step):
        return remote(
            block_source(job, step), block_home(job).at[c, slot(step, c)],
            core_send.at[job, step], core_recv.at[job, step], partner,
        )

    def extra_copy(job, first, lane):
        home = block_home(job).at[c, 4]
        src = (p_ref if job == 0 else m_ref).at[unchosen] if first else home
        target = above if lane == 0 else partner
        return remote(src, home, extra_send.at[job, lane], extra_recv.at[job, lane], target)

    def own_loads(job):
        ref = p_ref if job == 0 else m_ref
        return (
            pltpu.make_async_copy(ref.at[chosen], panel.at[c, slot(0, c)], load_sem.at[job, 0]),
            pltpu.make_async_copy(ref.at[unchosen], panel.at[c, 4], load_sem.at[job, 1]),
        )

    def begin_blocks(job):
        ring_copy(job, 0).start()

        @pl.when(offset == 0)
        def _():
            extra_copy(job, True, 0).start()
            extra_copy(job, True, 1).start()

        core_copy(job, 0).start()

    def step_blocks(job, step):
        wait_for(block_home(job).at[c, slot(step, c)], ring_recv.at[job, step - 1])
        if step < layers - 1:
            ring_copy(job, step).start()

        @pl.when(offset == step)
        def _():
            wait_for(block_home(job).at[c, 4], extra_recv.at[job, 0])
            if step < layers - 1:
                extra_copy(job, False, 0).start()
            extra_copy(job, False, 1).start()

        core_copy(job, step).start()

    def end_sends(job):
        for step in range(layers - 1):
            ring_copy(job, step).wait_send()
        for step in range(layers):
            core_copy(job, step).wait_send()

        @pl.when(offset < layers - 1)
        def _():
            extra_copy(job, False, 0).wait_send()

        extra_copy(job, False, 1).wait_send()

    def wait_core(job):
        for step in range(layers):
            wait_for(block_home(job).at[1 - c, slot(step, 1 - c)], core_recv.at[job, step])
        wait_for(block_home(job).at[1 - c, 4], extra_recv.at[job, 1])


    def start_copy(t, target_x, xr):
        columns = pl.ds(pl.multiple_of(mod(target_x + t, 2) * half, half), half)
        side = jnp.where(xr == target_x, 0, 1)
        src = s_ref.at[pl.ds(xr * w, w), columns]
        return src, cols.at[t, 2 + c + 2 * side], (t, c, xr)

    def start_sends(t):
        for xr in range(2):
            src, dst, at = start_copy(t, 1 - x, xr)
            remote(src, dst, start_send.at[t, 0, xr], start_recv.at[at], place(y, x, z, 1 - x)).start()

    def start_local(t):
        for xr in range(2):
            src, dst, at = start_copy(t, x, xr)

            @pl.when(c == x)
            def _():
                pltpu.make_async_copy(src, dst, start_recv.at[at]).start()

            @pl.when(c != x)
            def _():
                remote(src, dst, start_send.at[t, 1, xr], start_recv.at[at], partner).start()

    def far_copy(job, t):
        return remote(
            cols.at[t, 2:4], cols.at[t, 0:2], far_send.at[job, t], far_recv.at[job, t], across_y
        )

    start_sends(1)
    begin_blocks(0)
    start_local(1)
    own_p, own_e = own_loads(0)
    own_p.start()

    @pl.when(offset == 0)
    def _():
        own_e.start()

    start_sends(0)
    start_local(0)

    def take_start(t):
        for k in range(2):
            for xr in range(2):
                wait_for(cols.at[t, 0], start_recv.at[t, k, xr])
        far_copy(0, t).start()

    step_blocks(0, 1)
    take_start(1)
    step_blocks(0, 2)
    take_start(0)
    step_blocks(0, 3)
    begin_blocks(1)

    own_p.wait()

    @pl.when(offset == 0)
    def _():
        own_e.wait()

    wait_core(0)


    tile = w // 3

    def dot(a, b):
        return jnp.dot(a, b, preferred_element_type=f32)

    def turned_dot(a, b):
        return lax.dot_general(a, b, (((0,), (0,)), ((), ())), preferred_element_type=f32)

    def multiply(t):
        def chunk(i, _):
            at = pl.ds(pl.multiple_of(i * tile, tile), tile)

            def turned(k, d, block):
                return turned_dot(panel[k, d, :, at], cols[t, block])

            for k in range(2):
                def times(d, e):
                    return dot(panel[k, d, at, :], cols[t, (e + 2) % 4])

                middle = times(2, k + 2)
                near = times(0, k) + times(1, k + 1)
                near += turned(1, 3, 5) if k == 0 else turned(0, 1, 2)
                away = times(3, k + 3) + times(4, k)
                near += jnp.where(y == 0, middle, 0.0)
                away += jnp.where(y == 1, middle, 0.0)
                if t == 1:
                    acc[4 + k, at, :] = near
                    give_x[2 + k, at, :] = away.astype(bf16)
                else:
                    acc[k, at, :] = near
                    acc[2 + k, at, :] = away
            give_y[t, 0, at, :] = (turned(0, 2, 2 + 2 * y) + turned(1, 1, 3)).astype(bf16)
            give_y[t, 1, at, :] = (turned(0, 3, 4) + turned(1, 2, 3 + 2 * y)).astype(bf16)
            return 0

        lax.fori_loop(0, w // tile, chunk, 0)

    def y_copy(job, t):
        return remote(give_y.at[t], got_y.at[t], y_send.at[job, t], y_recv.at[job, t], across_y)

    def x_copy(job, s):
        return remote(
            give_x.at[2 * s : 2 * s + 2], got_x.at[2 - 2 * s : 4 - 2 * s],
            x_send.at[job, s], x_recv.at[job, 1 - s], across_x,
        )

    def over_rows(blocks, work):
        parts = 4
        size = w // parts

        def chunk(i, _):
            b = i // parts
            at = pl.ds(pl.multiple_of(lax.rem(i, parts) * size, size), size)
            work(b, at)
            return 0

        lax.fori_loop(0, blocks * parts, chunk, 0)

    def after_first(job):
        y_copy(job, 1).start()
        x_copy(job, 1).start()

    def add_and_give(job):
        wait_for(got_y.at[1], y_recv.at[job, 1])

        def work(k, at):
            give_x[k, at, :] = (acc[4 + k, at, :] + got_y[1, k, at, :].astype(f32)).astype(bf16)

        over_rows(2, work)
        x_copy(job, 0).start()

    def near_sum(k, at):
        return acc[k, at, :] + got_x[k, at, :].astype(f32) + got_y[0, k, at, :].astype(f32)

    def away_sum(k, at):
        return acc[2 + k, at, :] + got_x[2 + k, at, :].astype(f32)

    def end_copies(job):
        for t in range(2):
            y_copy(job, t).wait_send()
            x_copy(job, t).wait_send()

    wait_for(cols.at[1, 0:2], far_recv.at[0, 1])
    multiply(1)
    far_copy(0, 1).wait_send()
    after_first(0)
    wait_for(cols.at[0, 0:2], far_recv.at[0, 0])
    multiply(0)
    far_copy(0, 0).wait_send()
    y_copy(0, 0).start()
    step_blocks(1, 1)
    add_and_give(0)


    sign = jnp.where(x == 0, 1.0, -1.0).astype(f32)
    own = 2 * z + c

    def half_copy(s):
        return remote(
            cols.at[0, 2 + 2 * s : 4 + 2 * s], cols.at[1, 4 - 2 * s : 6 - 2 * s],
            half_send.at[s], half_recv.at[1 - s], across_x,
        )

    def put_basis(block, at, change):
        value = ((cols[0, 2 + block, at, :].astype(f32) + sign * change) * 0.5).astype(bf16)
        cols[0, 2 + block, at, :] = value
        line[own, block, at, :] = value

    wait_for(got_y.at[0], y_recv.at[0, 0])
    wait_for(got_x.at[0:2], x_recv.at[0, 0])
    over_rows(2, lambda k, at: put_basis(k, at, near_sum(k, at)))
    half_copy(0).start()
    far_copy(1, 0).start()
    step_blocks(1, 2)
    wait_for(got_x.at[2:4], x_recv.at[0, 1])
    over_rows(2, lambda k, at: put_basis(2 + k, at, away_sum(k, at)))
    half_copy(1).start()
    end_copies(0)


    def line_copy(step):
        at = 2 * mod(z - step, layers) + c
        return remote(line.at[at], line.at[at], line_send.at[step], line_recv.at[step], above)

    def pair_copy(step):
        at = 2 * mod(z - step, layers) + c
        return remote(line.at[at], line.at[at], pair_send.at[step], pair_recv.at[step], partner)

    def step_line(step):
        wait_for(line.at[0], line_recv.at[step - 1])
        if step < layers - 1:
            line_copy(step).start()
        pair_copy(step).start()

    step_blocks(1, 3)
    line_copy(0).start()
    pair_copy(0).start()

    end_sends(0)
    own_m, own_e = own_loads(1)
    own_m.start()

    @pl.when(offset == 0)
    def _():
        own_e.start()

    def staged(k, d, at):
        return pltpu.make_async_copy(stage_ref.at[k, d], panel.at[k, d], load_sem.at[at])

    for step in range(1, layers):
        staged(c, slot(step, c), (2, step)).start()

    @pl.when(offset != 0)
    def _():
        staged(c, 4, (1, 1)).start()

    wait_core(1)
    for step in range(layers):
        staged(1 - c, slot(step, 1 - c), (3, step)).start()
    staged(1 - c, 4, (2, 0)).start()

    wait_for(cols.at[1, 2:4], half_recv.at[0])
    wait_for(cols.at[1, 4:6], half_recv.at[1])
    far_copy(1, 1).start()

    own_m.wait()
    wait_for(panel.at[c, 4], load_sem.at[1, 1])
    for step in range(1, layers):
        staged(c, slot(step, c), (2, step)).wait()
    for step in range(layers):
        staged(1 - c, slot(step, 1 - c), (3, step)).wait()
    staged(1 - c, 4, (2, 0)).wait()

    wait_for(cols.at[0, 0:2], far_recv.at[1, 0])
    multiply(0)
    y_copy(1, 0).start()
    wait_for(cols.at[1, 0:2], far_recv.at[1, 1])
    multiply(1)
    after_first(1)
    step_line(1)
    add_and_give(1)
    for s in range(2):
        half_copy(s).wait_send()
        far_copy(1, s).wait_send()

    def put_image(block, at, value):
        cols[1, 2 + block, at, :] = value.astype(bf16)

    wait_for(got_y.at[0], y_recv.at[1, 0])
    wait_for(got_x.at[0:2], x_recv.at[1, 0])
    over_rows(2, lambda k, at: put_image(k, at, near_sum(k, at)))
    step_line(2)
    wait_for(got_x.at[2:4], x_recv.at[1, 1])
    over_rows(2, lambda k, at: put_image(2 + k, at, away_sum(k, at)))
    end_copies(1)


    def term_copy(which, v):
        return remote(
            give_x.at[2 * which + v], got_far.at[2 * which + v],
            term_send.at[which, v], term_recv.at[which, v], across_y,
        )

    def terms(step):
        layer = mod(z - step, layers)
        v = lax.rem(layer, 2)
        kept = layer // 2 == y
        if step > 0:
            wait_for(line.at[0], pair_recv.at[step])
        else:
            wait_for(line.at[0], pair_recv.at[0])

        def chunk(i, _):
            which, core = i // 2, lax.rem(i, 2)
            left = line[2 * layer + core].reshape(4 * w, half)
            right = cols[which, 2:6].reshape(4 * w, half)
            value = turned_dot(left, right)
            at = pl.ds(pl.multiple_of(core * half, half), half)

            @pl.when(kept)
            def _():
                acc[2 * which + v, at, :] = value

            @pl.when(jnp.logical_not(kept))
            def _():
                give_x[2 * which + v, at, :] = value.astype(bf16)

            return 0

        lax.fori_loop(0, 4, chunk, 0)

        @pl.when(jnp.logical_not(kept))
        def _():
            for which in range(2):
                term_copy(which, v).start()

    for step in range(layers - 1):
        terms(step)
    step_line(layers - 1)
    terms(layers - 1)

    outs = (gram_ref, proj_ref)
    to_half = pl.ds(pl.multiple_of(x * half, half), half)

    def out_copy(which, v):
        return remote(
            got_far.at[2 * which + v], outs[which].at[:, to_half],
            out_send.at[which, v], out_recv.at[which, x], place(y, v, z, c),
        )

    for which in range(2):
        for v in range(2):
            at = 2 * which + v
            wait_for(got_far.at[0], term_recv.at[which, v])

            def work(b, rows_at, at=at):
                total = acc[at, rows_at, :] + got_far[at, rows_at, :].astype(f32)
                got_far[at, rows_at, :] = total.astype(bf16)

            over_rows(1, work)
            local = jnp.logical_and(c == v, x == c)

            @pl.when(local)
            def _():
                pltpu.make_async_copy(
                    got_far.at[at], outs[which].at[:, to_half], out_recv.at[which, x]
                ).start()

            @pl.when(jnp.logical_not(local))
            def _():
                out_copy(which, v).start()


    for t in range(2):
        for xr in range(2):
            src, dst, at = start_copy(t, 1 - x, xr)
            remote(src, dst, start_send.at[t, 0, xr], start_recv.at[at], place(y, x, z, 1 - x)).wait_send()
            src, dst, at = start_copy(t, x, xr)

            @pl.when(c != x)
            def _():
                remote(src, dst, start_send.at[t, 1, xr], start_recv.at[at], partner).wait_send()

    end_sends(1)
    for step in range(layers - 1):
        line_copy(step).wait_send()
    for step in range(layers):
        pair_copy(step).wait_send()
    for which in range(2):
        for v in range(2):
            term_copy(which, v).wait_send()

            @pl.when(jnp.logical_not(jnp.logical_and(c == v, x == c)))
            def _():
                out_copy(which, v).wait_send()

        for h in range(2):
            wait_for(got_far.at[0], out_recv.at[which, h])


def plane_plan(matrix, polar_factor, start_basis):
    rows, w = start_basis.shape
    half = w // 2
    layers = lax.axis_size("col") // 2
    bf16, f32 = jnp.bfloat16, jnp.float32
    dma = pltpu.SemaphoreType.DMA
    any_space = pl.BlockSpec(memory_space=pl.ANY)
    out = jax.ShapeDtypeStruct((w, w), bf16)
    work = 2 * (rows * lax.axis_size("row")) ** 3 // (4 * lax.axis_size("col")) * 3
    gram, projected, _ = pl.pallas_call(
        plane_kernel,
        out_shape=(out, out, jax.ShapeDtypeStruct((2, 5, w, w), bf16)),
        in_specs=[any_space] * 3,
        out_specs=(any_space,) * 3,
        scratch_shapes=[
            pltpu.VMEM((2, 5, w, w), bf16),
            pltpu.VMEM((2 * layers, 4, w, half), bf16),
            pltpu.VMEM((2, 6, w, half), bf16),
            pltpu.VMEM((6, w, half), f32),
            pltpu.VMEM((4, w, half), bf16),
            pltpu.VMEM((4, w, half), bf16),
            pltpu.VMEM((2, 2, w, half), bf16),
            pltpu.VMEM((2, 2, w, half), bf16),
            pltpu.VMEM((4, w, half), bf16),
            dma((2, 2, 2)), dma((2, 2, 2)), dma((2, 2)), dma((2, 2)),
            dma((2, 3)), dma((2, 3)), dma((2, 4)), dma((2, 4)),
            dma((2, 2)), dma((2, 2)), dma((4, 4)), dma((2, 2)), dma((2, 2)),
            dma((2, 2)), dma((2, 2)), dma((2,)), dma((2,)),
            dma((3,)), dma((3,)), dma((4,)), dma((4,)),
            dma((2, 2)), dma((2, 2)), dma((2, 2)), dma((2, 2)),
        ],
        compiler_params=pltpu.CompilerParams(
            collective_id=0, has_side_effects=True, vmem_limit_bytes=63 * 1024 * 1024
        ),
        cost_estimate=pl.CostEstimate(
            flops=work, bytes_accessed=16 * rows * w, transcendentals=0
        ),
    )(matrix, polar_factor, start_basis)
    return gram.astype(f32), projected.astype(f32)


def solution(mesh):
    n_row, n_col = mesh.shape["row"], mesh.shape["col"]
    planes = n_row == 2 * 2 and n_col == 2 * n_row
    return jax.shard_map(
        plane_plan if planes else ring_plan,
        mesh=mesh,
        in_specs=(P("row", "col"), P("row", "col"), P("row", "col")),
        out_specs=(P("row", "col"), P("row", "col")),
        check_vma=False,
    )
```

```python
import jax
import jax.numpy as jnp
from jax import lax
from jax.experimental import pallas as pl
from jax.experimental.pallas import tpu as pltpu
from jax.sharding import PartitionSpec as P

MESH = pl.DeviceIdType.MESH


def ring_member(place, count):
    return jnp.where(place < count // 2, 2 * place, 2 * (count - 1 - place) + 1)


def ring_pairs(count):
    order = list(range(0, count, 2)) + list(range(count - 1, 0, -2))
    up = [(order[i], order[(i + 1) % count]) for i in range(count)]
    return up, [(b, a) for a, b in up]


def ring(first, second, count, consume, state, tie_from, hold=None):
    here = lax.axis_index("col")
    place = jnp.where(here % 2 == 0, here // 2, count - 1 - here // 2)
    up, down = ring_pairs(count)
    seen = []
    for step in range(count):
        if hold is not None and step == 2:
            first, second, _ = lax.optimization_barrier((first, second, hold))
        if step < count - 1:
            next_first = lax.ppermute(first, "col", up)
            next_second = lax.ppermute(second, "col", down)
        owner_first = ring_member(lax.rem(place - step + count, count), count)
        owner_second = ring_member(lax.rem(place + step, count), count)
        state = consume(state, first, owner_first, second, owner_second)
        seen.append(first)
        if tie_from <= step < count - 1:
            next_first, next_second, state = lax.optimization_barrier(
                (next_first, next_second, state)
            )
        first, second = next_first, next_second
    return state, seen


def block_row_product(block, columns, count, half_rows, tie_from, hold=None):
    depth = block.shape[1]

    def consume(state, top, owner_top, bottom, owner_bottom):
        pieces = []
        for total, piece, owner in ((state[0], top, owner_top), (state[1], bottom, owner_bottom)):
            rows = lax.dynamic_slice_in_dim(columns, owner * depth, depth, 0)
            term = jnp.dot(piece, rows, preferred_element_type=jnp.float32)
            pieces.append(term if total is None else total + term)
        return tuple(pieces)

    return ring(
        block[:half_rows], block[half_rows:], count, consume, (None, None), tie_from, hold
    )


def transposed_product(left, right):
    return lax.dot_general(
        left, right, (((0,), (0,)), ((), ())), preferred_element_type=jnp.float32
    )


def ring_plan(matrix, polar_factor, start_basis):
    local_rows, width = start_basis.shape
    count = lax.axis_size("col")
    half = width // 2
    half_rows = local_rows // 2
    sign = jnp.where(jnp.arange(width) < half, 1.0, -1.0).astype(jnp.float32)

    start_cols = lax.all_gather(start_basis, "row", axis=0, tiled=True)
    (top, bottom), polar_seen = block_row_product(
        polar_factor, start_cols, count, half_rows, count // 2
    )
    product = jnp.concatenate([top, bottom], axis=0)
    basis = ((start_basis.astype(jnp.float32) + sign * product) * 0.5).astype(jnp.bfloat16)
    basis_cols = lax.all_gather(basis, "row", axis=0, tiled=True)

    def keep(state, first, owner_first, second, owner_second):
        return (
            lax.dynamic_update_slice_in_dim(state[0], first, owner_first * half, 1),
            lax.dynamic_update_slice_in_dim(state[1], second, owner_second * half, 1),
        )

    empty = jnp.zeros((local_rows, half * count), jnp.bfloat16)
    lefts, seen = ring(basis[:, :half], basis[:, half:], count, keep, (empty, empty), count)

    matrix, _ = lax.optimization_barrier((matrix, polar_seen[-1]))
    halves, _ = block_row_product(
        matrix, basis_cols, count, half_rows, 2, seen[count // 2]
    )
    image = jnp.concatenate(halves, axis=0).astype(jnp.bfloat16)

    def summed(right):
        terms = [
            transposed_product(lefts[0], right[:, :half]),
            transposed_product(lefts[1], right[:, half:]),
        ]
        return lax.psum_scatter(
            jnp.concatenate(terms, axis=1).astype(jnp.bfloat16),
            "row",
            scatter_dimension=0,
            tiled=True,
        ).astype(jnp.float32)

    return summed(basis), summed(image)


def wait_for(ref, sem):
    pltpu.make_async_copy(ref, ref, sem).wait()


def plane_kernel(
    m_ref, p_ref, s_ref, gram_ref, proj_ref, stage_ref,
    panel, extra, line, cols, acc, sums, give_x, got_x, give_y, got_y, got_far, got_back,
    start_send, start_recv, far_send, far_recv, ring_send, ring_recv, core_send, core_recv,
    extra_send, extra_recv, load_sem, y_send, y_recv, x_send, x_recv, half_send, half_recv,
    line_send, line_recv, pair_send, pair_recv, term_send, term_recv, out_send, out_recv,
    back_send, back_recv, down_send, down_recv,
):
    rows, w = s_ref.shape
    half = w // 2
    row, col = lax.axis_index("row"), lax.axis_index("col")
    layers = line.shape[0] // 2
    y, c, z, x = row // 2, lax.rem(row, 2), col // 2, lax.rem(col, 2)
    q = row
    f32, bf16 = jnp.float32, jnp.bfloat16

    def mod(value, count):
        return lax.rem(value + count, count)

    def place(a, b, d, e):
        return (2 * a + b, 2 * d + e)

    across_x = place(y, c, z, 1 - x)
    across_y = place(1 - y, c, z, x)
    partner = place(y, 1 - c, z, x)
    crossed = place(y, 1 - c, z, 1 - x)
    above = place(y, c, mod(z + 1, layers), x)
    below = place(y, c, mod(z - 1, layers), x)

    def remote(src, dst, send, recv, target):
        return pltpu.make_async_remote_copy(
            src_ref=src, dst_ref=dst, send_sem=send, recv_sem=recv,
            device_id=target, device_id_type=MESH,
        )

    barrier = pltpu.get_barrier_semaphore()
    everyone = [across_x, across_y, partner, crossed]
    for move in (1, -1):
        for other_core in (c, 1 - c):
            for other_x in (x, 1 - x):
                everyone.append(place(y, other_core, mod(z + move, layers), other_x))
    for target in everyone:
        pl.semaphore_signal(barrier, inc=1, device_id=target, device_id_type=MESH)
    pl.semaphore_wait(barrier, len(everyone))

    offset = mod(z - q, layers)
    pick = jnp.where(offset < 2, 0, jnp.where(offset == 2, y, 1))
    chosen = pl.ds(pl.multiple_of(mod(x + pick, 2) * w, w), w)

    def slot(layer, core):
        return mod(layer - (2 * y + core), layers)


    def block_home(job):
        return panel if job == 0 else stage_ref

    def block_source(job, layer, first):
        if first:
            return (p_ref if job == 0 else m_ref).at[chosen]
        return block_home(job).at[c, slot(layer, c)]

    def line_hop(job, way, step):
        layer = z - step if way == 0 else z + step
        return remote(
            block_source(job, layer, step == 0), block_home(job).at[c, slot(layer, c)],
            ring_send.at[job, way, step], ring_recv.at[job, way, step], (above, below)[way],
        )

    def core_copy(job, layer, first=False):
        return remote(
            block_source(job, layer, first), block_home(job).at[c, slot(layer, c)],
            core_send.at[job, layer], core_recv.at[job, layer], partner,
        )

    can_go = (z < layers - 1, z > 0)

    def comes(way, step):
        return z >= step if way == 0 else z + step < layers

    def extra_source(job, r):
        top = pl.multiple_of((1 - x) * w + r * half, half)
        left = pl.multiple_of(mod(r + x, 2) * half, half)
        return (p_ref if job == 0 else m_ref).at[pl.ds(top, half), pl.ds(left, half)]

    goes_up = jnp.logical_and(z >= q, z < layers - 1)
    goes_down = jnp.logical_and(z <= q, z > 0)

    def extra_copy(job, first, lane, r):
        home = extra.at[job, c, r]
        return remote(
            extra_source(job, r) if first else home, home, extra_send.at[job, lane, r],
            extra_recv.at[job, lane // 2, r], (above, below, partner)[lane],
        )

    def pass_extra(job, first):
        for r in range(2):
            @pl.when(goes_up)
            def _():
                extra_copy(job, first, 0, r).start()

            @pl.when(goes_down)
            def _():
                extra_copy(job, first, 1, r).start()

            extra_copy(job, first, 2, r).start()

    def own_load(job):
        ref = p_ref if job == 0 else m_ref
        return pltpu.make_async_copy(ref.at[chosen], panel.at[c, slot(z, c)], load_sem.at[job, 0])

    def own_extra(job, r):
        return pltpu.make_async_copy(extra_source(job, r), extra.at[job, c, r], load_sem.at[job, 1 + r])

    def begin_blocks(job):
        for way in range(2):
            @pl.when(can_go[way])
            def _():
                line_hop(job, way, 0).start()

        @pl.when(z == q)
        def _():
            pass_extra(job, True)
            for r in range(2):
                own_extra(job, r).start()

        core_copy(job, z, True).start()

    def step_blocks(job, step):
        for way in range(2):
            @pl.when(comes(way, step))
            def _():
                layer = z - step if way == 0 else z + step
                wait_for(block_home(job).at[c, slot(layer, c)], ring_recv.at[job, way, step - 1])

                @pl.when(can_go[way])
                def _():
                    line_hop(job, way, step).start()

                core_copy(job, layer).start()

    def step_extra(job, step):
        @pl.when(jnp.logical_or(z - q == step, q - z == step))
        def _():
            for r in range(2):
                wait_for(extra.at[job, c, r], extra_recv.at[job, 0, r])
            pass_extra(job, False)

    def end_sends(job):
        for way in range(2):
            for step in range(layers - 1):
                @pl.when(jnp.logical_and(can_go[way], comes(way, step)))
                def _():
                    line_hop(job, way, step).wait_send()
        for layer in range(layers):
            core_copy(job, layer).wait_send()
        for r in range(2):
            @pl.when(goes_up)
            def _():
                extra_copy(job, False, 0, r).wait_send()

            @pl.when(goes_down)
            def _():
                extra_copy(job, False, 1, r).wait_send()

            extra_copy(job, False, 2, r).wait_send()

    def wait_core(job):
        for layer in range(layers):
            wait_for(block_home(job).at[1 - c, slot(layer, 1 - c)], core_recv.at[job, layer])
        for r in range(2):
            wait_for(extra.at[job, 1 - c, r], extra_recv.at[job, 1, r])

        @pl.when(z == q)
        def _():
            for r in range(2):
                own_extra(job, r).wait()


    def start_copy(t, target_x, xr):
        columns = pl.ds(pl.multiple_of(mod(target_x + t, 2) * half, half), half)
        side = jnp.where(xr == target_x, 0, 1)
        src = s_ref.at[pl.ds(xr * w, w), columns]
        return src, cols.at[t, 2 + c + 2 * side], (t, c, xr)

    def start_sends(t):
        for xr in range(2):
            src, dst, at = start_copy(t, 1 - x, xr)
            remote(src, dst, start_send.at[t, 0, xr], start_recv.at[at], place(y, x, z, 1 - x)).start()

    def start_local(t):
        for xr in range(2):
            src, dst, at = start_copy(t, x, xr)

            @pl.when(c == x)
            def _():
                pltpu.make_async_copy(src, dst, start_recv.at[at]).start()

            @pl.when(c != x)
            def _():
                remote(src, dst, start_send.at[t, 1, xr], start_recv.at[at], partner).start()

    def far_copy(job, t):
        return remote(
            cols.at[t, 2:4], cols.at[t, 0:2], far_send.at[job, t], far_recv.at[job, t], across_y
        )

    start_sends(1)
    begin_blocks(0)
    start_local(1)
    own_load(0).start()
    start_sends(0)
    start_local(0)

    def take_start(t):
        for k in range(2):
            for xr in range(2):
                wait_for(cols.at[t, 0], start_recv.at[t, k, xr])
        far_copy(0, t).start()

    step_blocks(0, 1)
    take_start(1)
    step_extra(0, 1)
    step_blocks(0, 2)
    take_start(0)
    step_extra(0, 2)
    step_blocks(0, 3)
    begin_blocks(1)
    step_extra(0, 3)

    own_load(0).wait()
    wait_core(0)


    tile = half

    def dot(a, b):
        return jnp.dot(a, b, preferred_element_type=f32)

    def turned_dot(a, b):
        return lax.dot_general(a, b, (((0,), (0,)), ((), ())), preferred_element_type=f32)

    def multiply(job, t):
        def chunk(i, _):
            at = pl.ds(pl.multiple_of(i * tile, tile), tile)
            twin = mod(i + x, 2)
            twin_at = pl.ds(pl.multiple_of(twin * tile, tile), tile)

            def turned(k, d, block):
                return turned_dot(panel[k, d, :, at], cols[t, block])

            for k in range(2):
                def times(d, e):
                    return dot(panel[k, d, at, :], cols[t, (e + 2) % 4])

                middle = times(2, k + 2)
                near = times(0, k) + times(1, k + 1)
                near += turned(1, 3, 5) if k == 0 else turned(0, 1, 2)
                near += turned_dot(extra[job, k, twin], cols[t, 4 + k, twin_at, :])
                away = times(3, k + 3) + dot(extra[job, k, i], cols[t, 2 + k, twin_at, :])
                near += jnp.where(y == 0, middle, 0.0)
                away += jnp.where(y == 1, middle, 0.0)
                if t == 1:
                    acc[4 + k, at, :] = near
                    give_x[2 + k, at, :] = away.astype(bf16)
                else:
                    acc[k, at, :] = near
                    acc[2 + k, at, :] = away
            give_y[t, 0, at, :] = (turned(0, 2, 2 + 2 * y) + turned(1, 1, 3)).astype(bf16)
            give_y[t, 1, at, :] = (turned(0, 3, 4) + turned(1, 2, 3 + 2 * y)).astype(bf16)
            return 0

        lax.fori_loop(0, w // tile, chunk, 0)

    def y_copy(job, t):
        return remote(give_y.at[t], got_y.at[t], y_send.at[job, t], y_recv.at[job, t], across_y)

    def x_copy(job, s):
        return remote(
            give_x.at[2 * s : 2 * s + 2], got_x.at[2 - 2 * s : 4 - 2 * s],
            x_send.at[job, s], x_recv.at[job, 1 - s], across_x,
        )

    def over_rows(blocks, work):
        parts = 4
        size = w // parts

        def chunk(i, _):
            b = i // parts
            at = pl.ds(pl.multiple_of(lax.rem(i, parts) * size, size), size)
            work(b, at)
            return 0

        lax.fori_loop(0, blocks * parts, chunk, 0)

    def after_first(job):
        y_copy(job, 1).start()
        x_copy(job, 1).start()

    def add_and_give(job):
        wait_for(got_y.at[1], y_recv.at[job, 1])

        def work(k, at):
            give_x[k, at, :] = (acc[4 + k, at, :] + got_y[1, k, at, :].astype(f32)).astype(bf16)

        over_rows(2, work)
        x_copy(job, 0).start()

    def near_sum(k, at):
        return acc[k, at, :] + got_x[k, at, :].astype(f32) + got_y[0, k, at, :].astype(f32)

    def away_sum(k, at):
        return acc[2 + k, at, :] + got_x[2 + k, at, :].astype(f32)

    def end_copies(job):
        for t in range(2):
            y_copy(job, t).wait_send()
            x_copy(job, t).wait_send()

    wait_for(cols.at[1, 0:2], far_recv.at[0, 1])
    multiply(0, 1)
    far_copy(0, 1).wait_send()
    after_first(0)
    wait_for(cols.at[0, 0:2], far_recv.at[0, 0])
    multiply(0, 0)
    far_copy(0, 0).wait_send()
    y_copy(0, 0).start()
    step_blocks(1, 1)
    add_and_give(0)
    step_extra(1, 1)


    sign = jnp.where(x == 0, 1.0, -1.0).astype(f32)
    own = 2 * z + c

    def half_copy(s):
        return remote(
            cols.at[0, 2 + 2 * s : 4 + 2 * s], cols.at[1, 4 - 2 * s : 6 - 2 * s],
            half_send.at[s], half_recv.at[1 - s], across_x,
        )

    def put_basis(block, at, change):
        value = ((cols[0, 2 + block, at, :].astype(f32) + sign * change) * 0.5).astype(bf16)
        cols[0, 2 + block, at, :] = value
        line[own, block, at, :] = value

    wait_for(got_y.at[0], y_recv.at[0, 0])
    wait_for(got_x.at[0:2], x_recv.at[0, 0])
    over_rows(2, lambda k, at: put_basis(k, at, near_sum(k, at)))
    far_copy(1, 0).start()
    step_blocks(1, 2)
    wait_for(got_x.at[2:4], x_recv.at[0, 1])
    over_rows(2, lambda k, at: put_basis(2 + k, at, away_sum(k, at)))
    half_copy(1).start()
    half_copy(0).start()
    end_copies(0)


    reach = layers // 2

    def line_copy(step):
        at = 2 * mod(z - step, layers) + c
        return remote(line.at[at], line.at[at], line_send.at[step], line_recv.at[step], above)

    def pair_copy(step):
        at = 2 * mod(z - step, layers) + c
        return remote(line.at[at], line.at[at], pair_send.at[step], pair_recv.at[step], partner)

    def step_line(step):
        wait_for(line.at[0], line_recv.at[step - 1])
        if step < reach:
            line_copy(step).start()
        pair_copy(step).start()

    step_extra(1, 2)

    @pl.when(z < layers - 1)
    def _():
        line_copy(0).start()

    pair_copy(0).start()
    wait_for(cols.at[1, 2:4], half_recv.at[0])
    far_copy(1, 1).start()

    @pl.when(z == layers - 1)
    def _():
        line_copy(0).start()

    step_blocks(1, 3)
    step_extra(1, 3)

    end_sends(0)
    own_load(1).start()
    def staged(k, d, at):
        return pltpu.make_async_copy(stage_ref.at[k, d], panel.at[k, d], load_sem.at[at])

    for step in range(1, layers):
        staged(c, slot(mod(z - step, layers), c), (2, step)).start()

    wait_core(1)
    for step in range(layers):
        staged(1 - c, slot(step, 1 - c), (3, step)).start()

    own_load(1).wait()
    for step in range(1, layers):
        staged(c, slot(mod(z - step, layers), c), (2, step)).wait()
    for step in range(layers):
        staged(1 - c, slot(step, 1 - c), (3, step)).wait()

    wait_for(cols.at[0, 0:2], far_recv.at[1, 0])
    multiply(1, 0)
    wait_for(cols.at[1, 4:6], half_recv.at[1])
    wait_for(cols.at[1, 0:2], far_recv.at[1, 1])
    multiply(1, 1)
    after_first(1)
    y_copy(1, 0).start()
    step_line(1)
    add_and_give(1)
    for s in range(2):
        half_copy(s).wait_send()
        far_copy(1, s).wait_send()

    def put_image(block, at, value):
        cols[1, 2 + block, at, :] = value.astype(bf16)


    def near_layer(v):
        return 2 * y + v

    def formed(layer):
        return mod(z - layer, layers) <= reach

    def term_copy(which, v):
        return remote(
            panel.at[0, 2 * which + v, :, 0:half], got_far.at[2 * which + v],
            term_send.at[which, v], term_recv.at[which, v], across_y,
        )

    def back_copy(which):
        return remote(
            panel.at[1, which, :, 0:half], got_back.at[which],
            back_send.at[which], back_recv.at[which], across_y,
        )

    def terms(which, step):
        layer = mod(z - step, layers)
        v = lax.rem(layer, 2)
        kept = layer // 2 == y

        def chunk(core, _):
            left = line[2 * layer + core].reshape(4 * w, half)
            right = cols[which, 2:6].reshape(4 * w, half)
            value = turned_dot(left, right)
            at = pl.ds(pl.multiple_of(core * half, half), half)

            @pl.when(kept)
            def _():
                sums[2 * which + v, at, :] = value

            @pl.when(jnp.logical_not(kept))
            def _():
                panel[0, 2 * which + v, at, 0:half] = value.astype(bf16)

            return 0

        lax.fori_loop(0, 2, chunk, 0)

        @pl.when(jnp.logical_not(kept))
        def _():
            term_copy(which, v).start()

    mine_back = z // 2 == y

    def back_terms(which):
        layer = mod(z - 1, layers)

        def chunk(core, _):
            left = cols[which, 2:6].reshape(4 * w, half)
            right = line[2 * layer + core].reshape(4 * w, half)
            value = turned_dot(left, right)
            at = pl.ds(pl.multiple_of(core * half, half), half)

            @pl.when(mine_back)
            def _():
                acc[4 + which, at, :] = value

            @pl.when(jnp.logical_not(mine_back))
            def _():
                panel[1, which, at, 0:half] = value.astype(bf16)

            return 0

        lax.fori_loop(0, 2, chunk, 0)

        @pl.when(jnp.logical_not(mine_back))
        def _():
            back_copy(which).start()

    outs = (gram_ref, proj_ref)
    to_half = pl.ds(pl.multiple_of(x * half, half), half)
    to_rows = pl.ds(pl.multiple_of(c * half, half), half)

    def down_copy(which, core):
        return remote(
            got_back.at[which, core * half : (core + 1) * half],
            outs[which].at[to_rows, to_half], down_send.at[which, core],
            down_recv.at[which, c, x], place(y, lax.rem(z, 2), mod(z - 1, layers), core),
        )

    def finish_back(which):
        @pl.when(mine_back)
        def _():
            wait_for(got_back.at[which], back_recv.at[which])

            def work(b, at):
                total = acc[4 + which, at, :] + got_back[which, at, :].astype(f32)
                got_back[which, at, :] = total.astype(bf16)

            over_rows(1, work)
            for core in range(2):
                down_copy(which, core).start()

    def out_copy(which, v):
        return remote(
            got_far.at[2 * which + v], outs[which].at[:, to_half],
            out_send.at[which, v], out_recv.at[which, x], place(y, v, z, c),
        )

    def finish(which, v, late):
        at = 2 * which + v
        local = jnp.logical_and(c == v, x == c)
        distance = mod(z - near_layer(v), layers)

        @pl.when(distance == reach if late else distance < reach)
        def _():
            wait_for(got_far.at[0], term_recv.at[which, v])

            def work(b, rows_at):
                total = sums[at, rows_at, :] + got_far[at, rows_at, :].astype(f32)
                got_far[at, rows_at, :] = total.astype(bf16)

            over_rows(1, work)

            @pl.when(local)
            def _():
                pltpu.make_async_copy(
                    got_far.at[at], outs[which].at[:, to_half], out_recv.at[which, x]
                ).start()

            @pl.when(jnp.logical_not(local))
            def _():
                out_copy(which, v).start()

    wait_for(line.at[0], pair_recv.at[0])
    wait_for(line.at[0], pair_recv.at[1])
    back_terms(0)
    terms(0, 1)
    terms(0, 0)
    wait_for(got_y.at[0], y_recv.at[1, 0])
    wait_for(got_x.at[0:2], x_recv.at[1, 0])
    over_rows(2, lambda k, at: put_image(k, at, near_sum(k, at)))
    wait_for(got_x.at[2:4], x_recv.at[1, 1])
    over_rows(2, lambda k, at: put_image(2 + k, at, away_sum(k, at)))
    end_copies(1)
    back_terms(1)
    terms(1, 1)
    terms(1, 0)
    finish_back(0)
    for step in range(2, reach + 1):
        step_line(step)
        wait_for(line.at[0], pair_recv.at[step])
        terms(1, step)
        terms(0, step)
    finish_back(1)
    for late in (False, True):
        for which in (late, not late):
            for v in range(2):
                finish(int(which), v, late)


    for t in range(2):
        for xr in range(2):
            src, dst, at = start_copy(t, 1 - x, xr)
            remote(src, dst, start_send.at[t, 0, xr], start_recv.at[at], place(y, x, z, 1 - x)).wait_send()
            src, dst, at = start_copy(t, x, xr)

            @pl.when(c != x)
            def _():
                remote(src, dst, start_send.at[t, 1, xr], start_recv.at[at], partner).wait_send()

    end_sends(1)
    for step in range(reach):
        line_copy(step).wait_send()
    for step in range(reach + 1):
        pair_copy(step).wait_send()
    for which in range(2):
        @pl.when(jnp.logical_not(mine_back))
        def _():
            back_copy(which).wait_send()

        @pl.when(mine_back)
        def _():
            for core in range(2):
                down_copy(which, core).wait_send()

        for v in range(2):
            @pl.when(formed(2 * (1 - y) + v))
            def _():
                term_copy(which, v).wait_send()

            @pl.when(jnp.logical_and(
                formed(near_layer(v)), jnp.logical_not(jnp.logical_and(c == v, x == c))
            ))
            def _():
                out_copy(which, v).wait_send()

        @pl.when(formed(q))
        def _():
            for h in range(2):
                wait_for(got_far.at[0], out_recv.at[which, h])

        @pl.when(jnp.logical_not(formed(q)))
        def _():
            for core in range(2):
                for h in range(2):
                    wait_for(got_back.at[0, 0:half], down_recv.at[which, core, h])


def plane_plan(matrix, polar_factor, start_basis):
    rows, w = start_basis.shape
    half = w // 2
    layers = lax.axis_size("col") // 2
    bf16, f32 = jnp.bfloat16, jnp.float32
    dma = pltpu.SemaphoreType.DMA
    any_space = pl.BlockSpec(memory_space=pl.ANY)
    out = jax.ShapeDtypeStruct((w, w), bf16)
    work = 2 * (rows * lax.axis_size("row")) ** 3 // (4 * lax.axis_size("col")) * 3
    gram, projected, _ = pl.pallas_call(
        plane_kernel,
        out_shape=(out, out, jax.ShapeDtypeStruct((2, layers, w, w), bf16)),
        in_specs=[any_space] * 3,
        out_specs=(any_space,) * 3,
        scratch_shapes=[
            pltpu.VMEM((2, layers, w, w), bf16),
            pltpu.VMEM((2, 2, 2, half, half), bf16),
            pltpu.VMEM((2 * layers, 4, w, half), bf16),
            pltpu.VMEM((2, 6, w, half), bf16),
            pltpu.VMEM((6, w, half), f32),
            pltpu.VMEM((4, w, half), f32),
            pltpu.VMEM((4, w, half), bf16),
            pltpu.VMEM((4, w, half), bf16),
            pltpu.VMEM((2, 2, w, half), bf16),
            pltpu.VMEM((2, 2, w, half), bf16),
            pltpu.VMEM((4, w, half), bf16),
            pltpu.VMEM((2, w, half), bf16),
            dma((2, 2, 2)), dma((2, 2, 2)), dma((2, 2)), dma((2, 2)),
            dma((2, 2, 3)), dma((2, 2, 3)), dma((2, 4)), dma((2, 4)),
            dma((2, 3, 2)), dma((2, 2, 2)), dma((4, 4)), dma((2, 2)), dma((2, 2)),
            dma((2, 2)), dma((2, 2)), dma((2,)), dma((2,)),
            dma((3,)), dma((3,)), dma((4,)), dma((4,)),
            dma((2, 2)), dma((2, 2)), dma((2, 2)), dma((2, 2)),
            dma((2,)), dma((2,)), dma((2, 2)), dma((2, 2, 2)),
        ],
        compiler_params=pltpu.CompilerParams(
            collective_id=0, has_side_effects=True, vmem_limit_bytes=63 * 1024 * 1024
        ),
        cost_estimate=pl.CostEstimate(
            flops=work, bytes_accessed=16 * rows * w, transcendentals=0
        ),
    )(matrix, polar_factor, start_basis)
    return gram.astype(f32), projected.astype(f32)


def solution(mesh):
    n_row, n_col = mesh.shape["row"], mesh.shape["col"]
    planes = n_row == 2 * 2 and n_col == 2 * n_row
    return jax.shard_map(
        plane_plan if planes else ring_plan,
        mesh=mesh,
        in_specs=(P("row", "col"), P("row", "col"), P("row", "col")),
        out_specs=(P("row", "col"), P("row", "col")),
        check_vma=False,
    )
```
